512 devices in a mesh: dp: 32 (over z, y_hi), seq: 16 (over y_lo, x, core).
Axes of the slice: x: 4, y: 8 (y_hi: 4, y_lo: 2; y = y_hi * 2 + y_lo), z: 8, core: 2. Of those that a mesh axis runs over, the one named last changes fastest.
Arguments:
- queries: bfloat16 [32, 2048, 2048], P('dp', 'seq'), may hold values from -5 to 5
- keys: bfloat16 [32, 2048, 2048], P('dp', 'seq'), may hold values from -5 to 5
- values: bfloat16 [32, 2048, 2048], P('dp', 'seq'), may hold values from -6 to 6
- stream: bfloat16 [32, 2048, 2048], P('dp', 'seq'), may hold values from -40 to 40
- layer_scale: float32 [2048], replicated, may hold values from 0.5 to 2
- norm_gain: float32 [2048], replicated, may hold values from 0.5 to 2
- teacher_gram: bfloat16 [32, 2048, 2048], P('dp', 'seq'), may hold values from -20 to 20, as said below
Outputs:
- feature_grad: bfloat16 [32, 2048, 2048], P('dp', 'seq')
- image_loss: float32 [32], P('dp')
- mean_loss: float32 [], replicated
The draws below stay inside these ranges and needn't reach their ends.
Inputs may be any that keep to these rules, and one draw needn't show every extreme that they name: Each image's teacher_gram is symmetric.
All inputs are finite; a program needn't handle non-finite values.
Results may differ from the reference program's by a relative error of at most 0.009.
Values may be sent and summed in bfloat16 or wider, within the bound.
No kernel may reach another device: no remote copies, remote signals or barrier semaphores. Data moves between devices by JAX's collectives and lax.ppermute only.
A program may use at most 64 MiB of HBM per device.

```python
import math
import jax
import jax.numpy as jnp
from jax import lax

HEADS = 32
HEAD_DIM = 64
WIDTH = 2048
TOKENS = 2048
IMAGES = 32


def query_key_pair(key):
    first_key = jax.random.fold_in(key, 101)
    second_key = jax.random.fold_in(key, 102)
    full_shape = (IMAGES, TOKENS, WIDTH)
    query_draw = 1.4 * jax.random.truncated_normal(first_key, -3.5, 3.5, full_shape, jnp.float32)
    key_draw = 1.4 * jax.random.truncated_normal(second_key, -3.5, 3.5, full_shape, jnp.float32)
    return (query_draw, key_draw)


def draw_queries(key, part):
    return query_key_pair(key)[0].astype(jnp.bfloat16)


def draw_keys(key, part):
    return query_key_pair(key)[1].astype(jnp.bfloat16)


def draw_stream(key, part):
    full_shape = (IMAGES, TOKENS, WIDTH)
    noise_key = jax.random.fold_in(key, 301)
    drawn = 0.2 * jax.random.truncated_normal(noise_key, -6.0, 6.0, full_shape, jnp.float32)
    return drawn.astype(jnp.bfloat16)


def draw_teacher_gram(key, part):
    noise_key = jax.random.fold_in(key, 201)
    full_shape = (IMAGES, TOKENS, TOKENS)
    position = jnp.arange(TOKENS, dtype=jnp.float32) / (TOKENS - 1)
    image_frac = jnp.arange(IMAGES, dtype=jnp.float32) / max(IMAGES - 1, 1)
    noise = jax.random.normal(noise_key, full_shape, jnp.float32)
    token_factor = jnp.sqrt(1.0 + 2.0 * position)
    symmetric = (noise + jnp.swapaxes(noise, 1, 2)) * (0.7071 / math.sqrt(WIDTH))
    row_factor = token_factor[None, :] * jnp.sqrt(jnp.sqrt(1.0 + 2.0 * image_frac))[:, None]
    gram = row_factor[:, :, None] * row_factor[:, None, :] * (symmetric + jnp.eye(TOKENS, dtype=jnp.float32)[None])
    return gram.astype(jnp.bfloat16)


def level_of(key, extent, pieces, low, high):
    gain = 1.0
    for dim, parts in pieces:
        draws = jax.random.uniform(jax.random.fold_in(jax.random.fold_in(key, 6), dim), (parts,), jnp.float32, low / len(pieces), high / len(pieces))
        gain = gain * jnp.repeat(jnp.exp(draws), extent[dim] // parts).reshape((-1,) + (1,) * (len(extent) - 1 - dim))
    return gain


def bell_draw(stream_key, dims, spread, bound, split=(), kind=jnp.bfloat16):
    loudness = level_of(stream_key, dims, split, -0.22, 0.18) if split else 1.0
    result = jax.random.normal(stream_key, dims, jnp.float32) * spread * loudness
    return jnp.minimum(jnp.maximum(result, -bound), bound).astype(kind)


def setup_inputs(seed: int = 0) -> dict:
    seeds = jax.random.split(jax.random.key(seed), 8)
    return {
        "queries": draw_queries(jax.random.fold_in(seeds[7], 71), 0),
        "keys": draw_keys(jax.random.fold_in(seeds[7], 71), 0),
        "values": bell_draw(seeds[2], (IMAGES, TOKENS, WIDTH), 1.0, 6.0, ((0, 32), (1, 16))),
        "stream": draw_stream(jax.random.fold_in(seeds[7], 71), 0),
        "layer_scale": jnp.clip(jnp.exp(jax.random.uniform(seeds[4], (WIDTH,), jnp.float32, math.log(0.5), math.log(2.0))), 0.5, 2.0),
        "norm_gain": jnp.clip(jnp.exp(jax.random.uniform(seeds[5], (WIDTH,), jnp.float32, math.log(0.5), math.log(2.0))), 0.5, 2.0),
        "teacher_gram": draw_teacher_gram(jax.random.fold_in(seeds[7], 71), 0),
    }


EPSILON = 1e-06

def attend_block(q_block, k_head, v_head):
    scores = jnp.einsum('qd,kd->qk', q_block, k_head, preferred_element_type=jnp.float32) / math.sqrt(q_block.shape[1])
    row_max = lax.optimization_barrier(jnp.max(scores, axis=1, keepdims=True))
    exponent = jnp.exp(scores - row_max)
    weights = (exponent / lax.optimization_barrier(jnp.sum(exponent, axis=1, keepdims=True))).astype(jnp.bfloat16)
    return jnp.dot(weights, v_head, preferred_element_type=jnp.float32).astype(jnp.bfloat16)

def attend_head(q_head, k_head, v_head):
    row_count, head_depth = q_head.shape
    block_rows = math.gcd(row_count, 512)
    blocks = q_head.reshape(row_count // block_rows, block_rows, head_depth)
    results = lax.map(lambda q_block: attend_block(q_block, k_head, v_head), blocks)
    return results.reshape(row_count, head_depth)

def forward_norm(summed, norm_gain):
    row_mean = lax.optimization_barrier(jnp.mean(summed, axis=-1, keepdims=True))
    centred = summed - row_mean
    variance = lax.optimization_barrier(jnp.mean(centred * centred, axis=-1, keepdims=True))
    inv_sigma = lax.rsqrt(variance + EPSILON)
    centred_hat = centred * inv_sigma
    normed = centred_hat * norm_gain
    inv_length = lax.rsqrt(lax.optimization_barrier(jnp.sum(normed * normed, axis=-1, keepdims=True)) + EPSILON)
    return (centred_hat, inv_sigma, normed, inv_length)

def backward_norm(cotangent, centred_hat, inv_sigma, normed, inv_length, norm_gain):
    along = lax.optimization_barrier(jnp.sum(normed * cotangent, axis=-1, keepdims=True))
    grad_normed = inv_length * cotangent - inv_length * inv_length * inv_length * normed * along
    scaled = grad_normed * norm_gain
    mean_scaled = lax.optimization_barrier(jnp.mean(scaled, axis=-1, keepdims=True))
    mean_product = lax.optimization_barrier(jnp.mean(scaled * centred_hat, axis=-1, keepdims=True))
    return (scaled - mean_scaled - centred_hat * mean_product) * inv_sigma

def one_image(inputs, layer_scale, norm_gain):
    image_q, image_k, image_v, image_stream, image_teacher = inputs
    split_q = jnp.transpose(image_q.reshape(TOKENS, HEADS, HEAD_DIM), (1, 0, 2))
    split_k = jnp.transpose(image_k.reshape(TOKENS, HEADS, HEAD_DIM), (1, 0, 2))
    split_v = jnp.transpose(image_v.reshape(TOKENS, HEADS, HEAD_DIM), (1, 0, 2))
    per_head = lax.map(lambda triple: attend_head(triple[0], triple[1], triple[2]), (split_q, split_k, split_v))
    attended = jnp.transpose(per_head, (1, 0, 2)).reshape(TOKENS, WIDTH)
    summed = image_stream.astype(jnp.float32) + layer_scale * attended.astype(jnp.float32)
    centred_hat, inv_sigma, normed, inv_length = forward_norm(summed, norm_gain)
    features = (normed * inv_length).astype(jnp.bfloat16)
    gram_diff = jnp.einsum('ad,bd->ab', features, features, preferred_element_type=jnp.float32) - image_teacher.astype(jnp.float32)
    image_loss = jnp.sum(gram_diff * gram_diff) * (WIDTH / (TOKENS * TOKENS))
    cotangent = jnp.dot(gram_diff.astype(jnp.bfloat16), features, preferred_element_type=jnp.float32) * (4.0 * WIDTH / (TOKENS * TOKENS))
    grad_summed = backward_norm(cotangent, centred_hat, inv_sigma, normed, inv_length, norm_gain)
    feature_grad = (grad_summed * (TOKENS * math.sqrt(WIDTH))).astype(jnp.bfloat16)
    return (feature_grad, image_loss)

def reference(queries, keys, values, stream, layer_scale, norm_gain, teacher_gram):
    feature_grad, image_loss = lax.map(lambda inputs: one_image(inputs, layer_scale, norm_gain), (queries, keys, values, stream, teacher_gram))
    mean_loss = jnp.mean(image_loss)
    return (feature_grad, image_loss, mean_loss)
```

```python
import math

import jax
import jax.numpy as jnp
from jax import lax
from jax.experimental import pallas as pl
from jax.experimental.pallas import tpu as pltpu
from jax.sharding import PartitionSpec as P

HEAD_DIM = 64
EPSILON = 1e-06
F32 = jnp.float32
BF16 = jnp.bfloat16


SEQ = 16
YC_GROUPS = [[base, base + 1, base + 8, base + 9] for base in (0, 2, 4, 6)]


def shifted(step):
    return [(s, (s & 9) | ((((s >> 1) + step) & 3) << 1)) for s in range(SEQ)]


RIGHT = shifted(1)
LEFT = shifted(3)


def exchanged(x, axis, groups=None):
    return lax.all_to_all(
        x, axis, split_axis=0, concat_axis=0, tiled=True, axis_index_groups=groups
    )


def attention_body(q_ref, kv_ref, out_ref, v_ref):
    width = 2 * HEAD_DIM
    low = lax.broadcasted_iota(jnp.int32, (1, width), 1) < HEAD_DIM

    @pl.when(pl.program_id(0) == 0)
    def _():
        v = kv_ref[:, 2 * width : 3 * width].astype(F32)
        v_ref[0] = jnp.where(low, v, 1.0).astype(BF16)
        v_ref[1] = jnp.where(low, 1.0, v).astype(BF16)

    q = q_ref[...].astype(F32)
    k = kv_ref[:, width : 2 * width]
    factor = math.log2(math.e) / math.sqrt(HEAD_DIM)
    results = []
    for head in range(2):
        mine = low if head == 0 else jnp.logical_not(low)
        q_head = jnp.where(mine, q, 0.0).astype(BF16)
        scores = lax.dot_general(
            q_head, k, (((1,), (1,)), ((), ())), preferred_element_type=F32
        )
        row_max = jnp.max(scores, axis=1, keepdims=True)
        weights = jnp.exp2((scores - row_max) * factor).astype(BF16)
        mixed = jnp.dot(weights, v_ref[head], preferred_element_type=F32)
        results.append(mixed / pltpu.roll(mixed, HEAD_DIM, 1))
    out_ref[...] = jnp.where(low, results[0], results[1]).astype(BF16)


def attention(packed, block_rows=256):
    rows = packed.shape[0]
    width = 2 * HEAD_DIM
    return pl.pallas_call(
        attention_body,
        out_shape=jax.ShapeDtypeStruct((rows, width), BF16),
        grid=(rows // block_rows,),
        in_specs=[
            pl.BlockSpec((block_rows, width), lambda i: (i, 0)),
            pl.BlockSpec((rows, 3 * width), lambda i: (0, 0)),
        ],
        out_specs=pl.BlockSpec((block_rows, width), lambda i: (i, 0)),
        scratch_shapes=[pltpu.VMEM((2, rows, width), BF16)],
        compiler_params=pltpu.CompilerParams(vmem_limit_bytes=48 * 1024 * 1024),
        name="attention",
    )(packed, packed)


def pack_body(q_ref, k_ref, v_ref, out_ref):
    for piece in range(out_ref.shape[0]):
        cols = slice(piece * 128, (piece + 1) * 128)
        out_ref[piece, :, 0:128] = q_ref[:, cols]
        out_ref[piece, :, 128:256] = k_ref[:, cols]
        out_ref[piece, :, 256:384] = v_ref[:, cols]


def packed_heads(q, k, v):
    rows, width = q.shape
    pieces = width // 128
    step = pieces // 4
    spec = pl.BlockSpec((rows, step * 128), lambda i: (0, i))
    return pl.pallas_call(
        pack_body,
        out_shape=jax.ShapeDtypeStruct((pieces, rows, 384), BF16),
        grid=(4,),
        in_specs=[spec] * 3,
        out_specs=pl.BlockSpec((step, rows, 384), lambda i: (i, 0, 0)),
        name="pack",
    )(q, k, v)


def norm_body(att_ref, stream_ref, scale_ref, gain_ref, feat_ref, hat_ref, stat_ref):
    pieces = att_ref.shape[0]
    att = jnp.concatenate([att_ref[i] for i in range(pieces)], axis=1).astype(F32)
    summed = stream_ref[...].astype(F32) + scale_ref[...] * att
    centred = summed - jnp.mean(summed, axis=1, keepdims=True)
    variance = jnp.mean(centred * centred, axis=1, keepdims=True)
    inv_sigma = lax.rsqrt(variance + EPSILON)
    hat = centred * inv_sigma
    normed = hat * gain_ref[...]
    inv_length = lax.rsqrt(jnp.sum(normed * normed, axis=1, keepdims=True) + EPSILON)
    feat_ref[...] = (normed * inv_length).astype(BF16)
    hat_ref[...] = hat
    wide = stat_ref.shape[1:]
    stat_ref[0] = jnp.broadcast_to(inv_sigma, wide)
    stat_ref[1] = jnp.broadcast_to(inv_length, wide)


def forward_norm(att, stream, scale, gain):
    rows, width = stream.shape
    pieces = att.shape[0]
    step = 32
    row = pl.BlockSpec((step, width), lambda i: (i, 0))
    flat = pl.BlockSpec((1, width), lambda i: (0, 0))
    return pl.pallas_call(
        norm_body,
        out_shape=(
            jax.ShapeDtypeStruct((rows, width), BF16),
            jax.ShapeDtypeStruct((rows, width), F32),
            jax.ShapeDtypeStruct((2, rows, 128), F32),
        ),
        grid=(rows // step,),
        in_specs=[pl.BlockSpec((pieces, step, 128), lambda i: (0, i, 0)), row, flat, flat],
        out_specs=(row, row, pl.BlockSpec((2, step, 128), lambda i: (0, i, 0))),
        name="norm",
    )(att, stream, scale, gain)


def gram_body(rows_ref, own_ref, left_ref, right_ref, far0_ref, far1_ref, taught_ref, diff_ref, loss_ref):
    group = pl.program_id(0)
    f = rows_ref[0]
    cols = (own_ref, left_ref, right_ref, far0_ref, far1_ref)
    start = 0
    total = jnp.zeros((1, 128), F32)
    for ref in cols:
        size = ref.shape[0]
        tile = lax.dot_general(
            f, ref[...], (((1,), (1,)), ((), ())), preferred_element_type=F32
        )
        differ = tile - taught_ref[0, :, start : start + size].astype(F32)
        diff_ref[0, :, start : start + size] = differ.astype(BF16)
        part = jnp.sum(differ * differ, axis=0, keepdims=True)
        total = total + jnp.sum(part)
        start += size

    @pl.when(group == 0)
    def _():
        loss_ref[...] = jnp.zeros(loss_ref.shape, F32)

    loss_ref[...] += jnp.broadcast_to(total, loss_ref.shape)


def gram_loss(rows, own, left, right, far0, far1, taught):
    groups, count, width = rows.shape
    cols = taught.shape[2]

    def whole(x):
        return pl.BlockSpec(x.shape, lambda i: (0,) * x.ndim)

    return pl.pallas_call(
        gram_body,
        out_shape=(
            jax.ShapeDtypeStruct((groups, count, cols), BF16),
            jax.ShapeDtypeStruct((SEQ, 128), F32),
        ),
        grid=(groups,),
        in_specs=[
            pl.BlockSpec((1, count, width), lambda i: (i, 0, 0)),
            whole(own),
            whole(left),
            whole(right),
            whole(far0),
            whole(far1),
            pl.BlockSpec((1, count, cols), lambda i: (i, 0, 0)),
        ],
        out_specs=(
            pl.BlockSpec((1, count, cols), lambda i: (i, 0, 0)),
            pl.BlockSpec((SEQ, 128), lambda i: (0, 0)),
        ),
        name="gram",
    )(rows, own, left, right, far0, far1, taught)


def pull_body(diff_ref, own_ref, left_ref, right_ref, far0_ref, far1_ref, out_ref):
    cols = (own_ref, left_ref, right_ref, far0_ref, far1_ref)
    start = 0
    total = None
    for ref in cols:
        size = ref.shape[0]
        term = jnp.dot(
            diff_ref[0, :, start : start + size], ref[...], preferred_element_type=F32
        )
        total = term if total is None else total + term
        start += size
    out_ref[0] = total.astype(BF16)


def pulled(diff, own, left, right, far0, far1):
    groups, count, cols = diff.shape
    width = own.shape[1]

    def whole(x):
        return pl.BlockSpec(x.shape, lambda i: (0,) * x.ndim)

    return pl.pallas_call(
        pull_body,
        out_shape=jax.ShapeDtypeStruct((groups, count, width), BF16),
        grid=(groups,),
        in_specs=[
            pl.BlockSpec((1, count, cols), lambda i: (i, 0, 0)),
            whole(own),
            whole(left),
            whole(right),
            whole(far0),
            whole(far1),
        ],
        out_specs=pl.BlockSpec((1, count, width), lambda i: (i, 0, 0)),
        name="pull",
    )(diff, own, left, right, far0, far1)


def backward_body(weight, scale_out, parts_ref, hat_ref, stat_ref, gain_ref, out_ref):
    gain = gain_ref[...]
    hat = hat_ref[...]
    total = parts_ref[0].astype(F32)
    for i in range(1, parts_ref.shape[0]):
        total = total + parts_ref[i].astype(F32)
    cotangent = total * weight
    inv_sigma = stat_ref[0][:, 0:1]
    inv_length = stat_ref[1][:, 0:1]
    normed = hat * gain
    along = jnp.sum(normed * cotangent, axis=1, keepdims=True)
    cube = inv_length * inv_length * inv_length
    scaled = (inv_length * cotangent - cube * along * normed) * gain
    mean_scaled = jnp.mean(scaled, axis=1, keepdims=True)
    mean_product = jnp.mean(scaled * hat, axis=1, keepdims=True)
    grad = (scaled - mean_scaled - hat * mean_product) * inv_sigma
    out_ref[...] = (grad * scale_out).astype(BF16)


def backward_norm(parts, hat, stat, gain, weight, scale_out):
    rows, width = hat.shape
    step = 32
    row = pl.BlockSpec((step, width), lambda i: (i, 0))

    def body(*refs):
        backward_body(weight, scale_out, *refs)

    return pl.pallas_call(
        body,
        out_shape=jax.ShapeDtypeStruct((rows, width), BF16),
        grid=(rows // step,),
        in_specs=[
            pl.BlockSpec((parts.shape[0], step, width), lambda i: (0, i, 0)),
            row,
            pl.BlockSpec((2, step, 128), lambda i: (0, i, 0)),
            pl.BlockSpec((1, width), lambda i: (0, 0)),
        ],
        out_specs=row,
        name="backward",
    )(parts, hat, stat, gain)


def local(queries, keys, values, stream, layer_scale, norm_gain, teacher_gram):
    tokens, width = queries.shape[1:]
    tokens_all = tokens * SEQ
    place = lax.axis_index("seq")
    gain = norm_gain.reshape(1, width)

    heads = exchanged(packed_heads(queries[0], keys[0], values[0]), "seq")

    x = (place >> 1) & 3
    teacher = teacher_gram[0].reshape(tokens, 2, 4, 2, tokens)
    order = (x + jnp.array([0, 3, 1, 2])) & 3
    teacher = jnp.take(teacher, order, axis=2)
    teacher = teacher.transpose(1, 3, 0, 2, 4).reshape(4, tokens, 4 * tokens)
    taught = exchanged(teacher, "seq", YC_GROUPS)

    attended_heads = attention(heads.reshape(tokens_all, 3 * 2 * HEAD_DIM))
    attended = exchanged(attended_heads.reshape(SEQ, tokens, 2 * HEAD_DIM), "seq")
    features, hat, stat = forward_norm(
        attended, stream[0], layer_scale.reshape(1, width), gain
    )

    half = tokens // 2
    rows = exchanged(jnp.broadcast_to(features, (4, tokens, width)), "seq", YC_GROUPS)
    left = lax.ppermute(features, "seq", RIGHT)
    right = lax.ppermute(features, "seq", LEFT)
    far0 = lax.ppermute(left[:half], "seq", RIGHT)
    far1 = lax.ppermute(right[half:], "seq", LEFT)

    diff, loss_part = gram_loss(rows, features, left, right, far0, far1, taught)
    image_total = jnp.sum(exchanged(loss_part, "seq"), axis=0, keepdims=True)
    image_loss = image_total * (width / (tokens_all * tokens_all))
    partials = pulled(diff, features, left, right, far0, far1)
    parts = exchanged(partials, "seq", YC_GROUPS)
    weight = 4.0 * width / (tokens_all * tokens_all)
    feature_grad = backward_norm(
        parts, hat, stat, gain, weight, tokens_all * math.sqrt(width)
    )
    images = lax.axis_size("dp")
    spread = exchanged(jnp.broadcast_to(image_loss, (images, 128)), "dp")
    mean_loss = jnp.sum(spread[:, 0]) / images
    return (feature_grad[None], image_loss[0, 0:1], mean_loss)


def solution(mesh):
    return jax.shard_map(
        local,
        mesh=mesh,
        in_specs=(
            P("dp", "seq", None),
            P("dp", "seq", None),
            P("dp", "seq", None),
            P("dp", "seq", None),
            P(),
            P(),
            P("dp", "seq", None),
        ),
        out_specs=(P("dp", "seq", None), P("dp"), P()),
        check_vma=False,
    )
```
